32 devices in a mesh: tm: 8 (over z, y), space: 4 (over x, core).
Axes of the slice: x: 2, y: 2, z: 4, core: 2. Of those that a mesh axis runs over, the one named last changes fastest.
Arguments:
- c_points: float32 [8, 64, 32, 128], P('tm', 'space'), may hold values from -15 to 15
- corrections: float32 [8, 64, 32, 128], P('tm', 'space'), may hold values from -3 to 3
- conductivity: float32 [64, 32, 128], P('space'), may hold values from 0.2 to 5
- forcing: float32 [64, 32, 128], P('space'), may hold values from -6 to 6
Outputs:
- f_states: float32 [8, 2, 64, 32, 128], P('tm', None, 'space')
The draws below stay inside these ranges and needn't reach their ends.
All inputs are finite; a program needn't handle non-finite values.
Results may differ from the reference program's by a relative error of at most 0.0002.
Values sent between devices are 32-bit elements; how exact they have to be, the bound alone decides.
A program may use at most 64 MiB of HBM per device.

```python
import math
import jax
import jax.numpy as jnp
from jax import lax

NY = 32
NX = 128
ITERS = 6
STEPS = 2
GROUPS = 8
NZ = 64


def draw_c_points(key, part):
    depth_frac = jnp.arange(NZ, dtype=jnp.float32) / max(NZ - 1, 1)
    depth_scale = (1.0 + 2.0 * depth_frac)[None, :, None, None]
    random_part = jax.random.normal(key, (GROUPS, NZ, NY, NX), jnp.float32)
    values = depth_scale * random_part
    return jnp.clip(values, -15.0, 15.0)


def block_levels(key, shape, cuts, smallest, largest):
    factor_of = 1.0
    for dim, parts in cuts:
        heights = jax.random.uniform(jax.random.fold_in(jax.random.fold_in(key, 6), dim), (parts,), jnp.float32, smallest / len(cuts), largest / len(cuts))
        factor_of = factor_of * jnp.repeat(jnp.exp(heights), shape[dim] // parts).reshape((-1,) + (1,) * (len(shape) - 1 - dim))
    return factor_of


def gaussian(key, extent, spread, most, shards=(), kind=jnp.bfloat16):
    factor_of = block_levels(key, extent, shards, -0.22, 0.18) if shards else 1.0
    entries = jax.random.normal(key, extent, jnp.float32) * spread * factor_of
    return jnp.minimum(jnp.maximum(entries, -most), most).astype(kind)


def setup_inputs(seed: int = 0) -> dict:
    keys = jax.random.split(jax.random.key(seed), 5)
    return {
        "c_points": draw_c_points(jax.random.fold_in(keys[4], 71), 0),
        "corrections": gaussian(keys[1], (GROUPS, NZ, NY, NX), 0.5, 3.0, ((0, 8), (1, 4)), jnp.float32),
        "conductivity": jnp.clip(jnp.exp(math.log(5.0) - 3.218876 * jax.random.uniform(keys[2], (NZ, NY, NX), jnp.float32) ** block_levels(keys[2], (NZ, NY, NX), ((0, 4),), -0.2, 0.2)), 0.2, 5.0),
        "forcing": gaussian(keys[3], (NZ, NY, NX), 1.0, 6.0, ((0, 4),), jnp.float32),
    }


step_rate = 4.0
source_weight = 0.25


def neighbours(padded):
    return (padded[2:, 1:-1, 1:-1], padded[:-2, 1:-1, 1:-1],
            padded[1:-1, 2:, 1:-1], padded[1:-1, :-2, 1:-1],
            padded[1:-1, 1:-1, 2:], padded[1:-1, 1:-1, :-2])


def faces_of(padded_conductivity):
    centre = padded_conductivity[1:-1, 1:-1, 1:-1]
    return tuple(0.5 * (centre + beside) for beside in neighbours(padded_conductivity))


def apply_operator(grid_field, padded, face_weights):
    flux_sum = jnp.zeros_like(grid_field)
    for face_weight, beside in zip(face_weights, neighbours(padded)):
        flux_sum = flux_sum + face_weight * (grid_field - beside)
    return grid_field + step_rate * flux_sum


def reference(c_points, corrections, conductivity, forcing):
    face_weights = faces_of(jnp.pad(conductivity, 1))

    def operate(grid_field):
        return apply_operator(grid_field, jnp.pad(grid_field, 1), face_weights)

    def advance(start_value):
        current = start_value
        sections = []
        for section in range(STEPS):
            right_side = current + source_weight * forcing
            solution = current
            residual = right_side - operate(current)
            direction = residual
            norm_now = jnp.sum(residual * residual)
            for sweep in range(ITERS):
                applied = operate(direction)
                step_length = norm_now / jnp.sum(direction * applied)
                solution = solution + step_length * direction
                if sweep + 1 < ITERS:
                    residual = residual - step_length * applied
                    norm_next = jnp.sum(residual * residual)
                    direction = residual + (norm_next / norm_now) * direction
                    norm_now = norm_next
            sections.append(solution)
            current = solution
        return jnp.stack(sections)

    prior_fix = jnp.concatenate([jnp.zeros_like(corrections[:1]), corrections[:-1]], axis=0)
    start_values = c_points + prior_fix
    return lax.map(advance, start_values)
```

```python
import functools

import jax
import jax.numpy as jnp
from jax import lax
from jax.experimental import pallas as pl
from jax.experimental.pallas import tpu as pltpu
from jax.sharding import PartitionSpec as P

ITERS = 6
STEPS = 2
STEP_RATE = 4.0
SOURCE_WEIGHT = 0.25
HALO = ITERS * STEPS + 1
OFF = HALO + 1
SUB = 8


def kernel(nt, ns, depth, rows, c_hbm, corr_hbm, cond_hbm, f_hbm, out_hbm,
           c_nat, g_nat, k_nat, f_nat, out_nat, x_buf, r_buf, w_buf, p_buf, q_buf, d_buf,
           dg, cx, cy, cz, slots, totals,
           in_sem, out_sem, corr_send, corr_recv, halo_send, halo_recv, red_send, red_recv):
    tm = lax.axis_index("tm")
    me = lax.axis_index("space")
    jn = rows // SUB
    top = OFF + depth
    planes = top + OFF
    half = 0.5 * STEP_RATE

    loads = [
        pltpu.make_async_copy(cond_hbm, k_nat.at[pl.ds(OFF, depth)], in_sem.at[0]),
        pltpu.make_async_copy(c_hbm.at[0], c_nat, in_sem.at[1]),
        pltpu.make_async_copy(f_hbm, f_nat.at[pl.ds(OFF, depth)], in_sem.at[2]),
    ]
    for load in loads:
        load.start()

    barrier = pltpu.get_barrier_semaphore()
    for other in range(1, ns):
        pl.semaphore_signal(barrier, inc=1, device_id={"space": lax.rem(me + other, ns)})

    @pl.when(tm > 0)
    def _():
        pl.semaphore_signal(barrier, inc=1, device_id={"tm": tm - 1})

    pl.semaphore_wait(barrier, ns - 1 + jnp.where(tm < nt - 1, 1, 0))

    corr = pltpu.make_async_remote_copy(
        src_ref=corr_hbm.at[0], dst_ref=g_nat, send_sem=corr_send, recv_sem=corr_recv,
        device_id={"tm": jnp.minimum(tm + 1, nt - 1)})

    @pl.when(tm < nt - 1)
    def _():
        corr.start()

    def halo(src, src_off, dst, width, slot):
        up = pltpu.make_async_remote_copy(
            src_ref=src.at[pl.ds(src_off + depth - width, width)],
            dst_ref=dst.at[pl.ds(OFF - width, width)],
            send_sem=halo_send.at[2 * slot], recv_sem=halo_recv.at[2 * slot],
            device_id={"space": jnp.minimum(me + 1, ns - 1)})
        down = pltpu.make_async_remote_copy(
            src_ref=src.at[pl.ds(src_off, width)],
            dst_ref=dst.at[pl.ds(top, width)],
            send_sem=halo_send.at[2 * slot + 1], recv_sem=halo_recv.at[2 * slot + 1],
            device_id={"space": jnp.maximum(me - 1, 0)})

        def start():
            pl.when(me < ns - 1)(up.start)
            pl.when(me > 0)(down.start)

        def wait():
            pl.when(me > 0)(up.wait_recv)
            pl.when(me < ns - 1)(down.wait_recv)

        def wait_send():
            pl.when(me < ns - 1)(up.wait_send)
            pl.when(me > 0)(down.wait_send)

        return start, wait, wait_send

    k_halo = halo(cond_hbm, 0, k_nat, HALO, 0)
    f_halo = halo(f_hbm, 0, f_nat, HALO - 1, 1)
    x_halo = halo(x_buf, OFF, x_buf, HALO, 2)
    k_halo[0]()
    f_halo[0]()

    zero_plane = jnp.zeros((rows, 128), jnp.float32)
    zero_tiles = jnp.zeros((jn, SUB, 128), jnp.float32)

    def clear(lo, count):
        def one(i, carry):
            k_nat[lo + i] = zero_plane
            f_nat[lo + i] = zero_plane
            x_buf[lo + i] = zero_tiles
            return carry
        lax.fori_loop(0, count, one, 0)

    clear(0, 1)
    clear(planes - 1, 1)
    pl.when(me == 0)(lambda: clear(1, HALO))
    pl.when(me == ns - 1)(lambda: clear(top, HALO))

    for buf in (r_buf, d_buf):
        buf[0] = zero_tiles
        buf[1] = zero_tiles
        buf[planes - 2] = zero_tiles
        buf[planes - 1] = zero_tiles

    lane = lax.broadcasted_iota(jnp.int32, (SUB, 128), 1)
    sub = lax.broadcasted_iota(jnp.int32, (SUB, 128), 0)
    inner_lane = jnp.where(lane < 127, 1.0, 0.0)
    first_lane = jnp.where(lane > 0, 1.0, 0.0)
    inner_sub = jnp.where(sub < SUB - 1, 1.0, 0.0)
    first_sub = jnp.where(sub > 0, 1.0, 0.0)

    def nat(ref, p, j):
        return ref[p, pl.ds(j, SUB, stride=jn), :]

    def ahead(x):
        return pltpu.roll(x, 127, 1)

    def behind(x):
        return pltpu.roll(x, 1, 1)

    def sub_ahead(x):
        return pltpu.roll(x, SUB - 1, 0)

    def sub_behind(x):
        return pltpu.roll(x, 1, 0)

    loads[0].wait()
    k_halo[1]()

    def make_weights(i, carry):
        p = i + 1
        k = [nat(k_nat, p, j) for j in range(jn)]
        up = [nat(k_nat, p + 1, j) for j in range(jn)]
        dn = [nat(k_nat, p - 1, j) for j in range(jn)]
        z = me * depth + p - OFF
        face = jnp.where((z >= 0) & (z + 1 < ns * depth), -half, 0.0)
        for j in range(jn):
            right = ahead(k[j]) * inner_lane
            left = behind(k[j]) * first_lane
            yp = k[j + 1] if j + 1 < jn else sub_ahead(k[0]) * inner_sub
            ym = k[j - 1] if j > 0 else sub_behind(k[jn - 1]) * first_sub
            around = right + left + yp + ym + up[j] + dn[j]
            dg[p, j] = 1.0 + half * (6.0 * k[j] + around)
            cx[p, j] = -half * (k[j] + right) * inner_lane
            wy = -half * (k[j] + yp)
            cy[p, j] = wy if j + 1 < jn else wy * inner_sub
            cz[p, j] = face * (k[j] + up[j])
        return carry

    lax.fori_loop(0, planes - 2, make_weights, 0)

    def apply(ref, p):
        v = [ref[p, j] for j in range(jn)]
        c = [cx[p, j] for j in range(jn)]
        y = [cy[p, j] for j in range(jn)]
        rolled = [ahead(v[j]) for j in range(jn)]
        back = [behind(c[j] * v[j]) for j in range(jn)]
        out = []
        for j in range(jn):
            acc = dg[p, j] * v[j] + cz[p, j] * ref[p + 1, j] + cz[p - 1, j] * ref[p - 1, j]
            acc = acc + y[j] * (v[j + 1] if j + 1 < jn else sub_ahead(v[0]))
            acc = acc + (y[j - 1] * v[j - 1] if j > 0 else sub_behind(y[jn - 1] * v[jn - 1]))
            out.append(acc + (c[j] * rolled[j] + back[j]))
        return out, v

    def both_halos(width, fn):
        count = (width + 1) // 2

        def step(i, carry):
            for t in range(2):
                fn(OFF - 1 - (2 * i + t))
                fn(top + 2 * i + t)
            return carry
        if count:
            lax.fori_loop(0, count, step, 0)

    def own(fn, carry, chunk=4):
        def step(i, carry):
            for t in range(chunk):
                carry = fn(OFF + i * chunk + t, carry)
            return carry
        return lax.fori_loop(0, depth // chunk, step, carry)

    loads[1].wait()

    @pl.when(tm > 0)
    def _():
        corr.wait_recv()

        def add(p, carry):
            for j in range(jn):
                x_buf[p, j] = nat(c_nat, p - OFF, j) + nat(g_nat, p - OFF, j)
            return carry
        own(add, 0)

    @pl.when(tm == 0)
    def _():
        def add(p, carry):
            for j in range(jn):
                x_buf[p, j] = nat(c_nat, p - OFF, j)
            return carry
        own(add, 0)

    x_halo[0]()
    loads[2].wait()
    f_halo[1]()

    def first_residual(p):
        image, v = apply(x_buf, p)
        for j in range(jn):
            r_buf[p, j] = (v[j] + SOURCE_WEIGHT * nat(f_nat, p, j)) - image[j]

    def first_own(i, carry):
        for t in range(2):
            first_residual(OFF + 1 + 2 * i + t)
        return carry

    lax.fori_loop(0, (depth - 2) // 2, first_own, 0)
    x_halo[1]()
    x_halo[2]()
    first_residual(OFF)
    first_residual(top - 1)
    both_halos(HALO - 1, first_residual)

    def spread(row):
        return jnp.broadcast_to(row, (SUB, 128))

    def reduce(stage, parts):
        for i, part in enumerate(parts):
            slots[stage, me, i:i + 1] = jnp.sum(part, axis=0, keepdims=True)
        for i in range(len(parts), SUB):
            slots[stage, me, i:i + 1] = jnp.zeros((1, 128), jnp.float32)
        copies = []
        for other in range(1, ns):
            copies.append(pltpu.make_async_remote_copy(
                src_ref=slots.at[stage, me], dst_ref=slots.at[stage, me],
                send_sem=red_send.at[stage, other], recv_sem=red_recv.at[stage, other],
                device_id={"space": lax.rem(me + other, ns)}))
        for copy in copies:
            copy.start()
        for copy in copies:
            copy.wait()
        total = slots[stage, 0]
        for i in range(1, ns):
            total = total + slots[stage, i]
        totals[stage] = jnp.broadcast_to(jnp.sum(total, axis=1, keepdims=True), (SUB, 128))
        return [spread(totals[stage, i:i + 1]) for i in range(len(parts))]

    zero = jnp.zeros((SUB, 128), jnp.float32)
    for section in range(STEPS):
        for sweep in range(ITERS):
            n = section * ITERS + sweep
            width = HALO - 2 - n

            def image_at(p):
                image, v = apply(r_buf, p)
                for j in range(jn):
                    w_buf[p, j] = image[j]
                return image, v

            def image_own(p, carry):
                rr, rw = carry
                image, v = image_at(p)
                for j in range(jn):
                    rr = rr + v[j] * v[j]
                    rw = rw + v[j] * image[j]
                return rr, rw

            rr, rw = reduce_in = own(image_own, (zero, zero))
            both_halos(width, image_at)
            norm, product = reduce(n, reduce_in)
            if sweep == 0:
                step_length = norm / product
                beta = None
            else:
                beta = norm / norm_before
                step_length = norm / (product - beta * norm / step_length)
            norm_before = norm
            last_sweep = sweep + 1 == ITERS
            last = last_sweep and section + 1 == STEPS

            def update(p, is_own):
                for j in range(jn):
                    r = r_buf[p, j]
                    pp = r if beta is None else r + beta * p_buf[p, j]
                    d = step_length * pp
                    if beta is not None:
                        d = d_buf[p, j] + d
                    if not last_sweep:
                        p_buf[p, j] = pp
                    if not last:
                        w = w_buf[p, j]
                        q = w if beta is None else w + beta * q_buf[p, j]
                        r = r - step_length * q
                        if last_sweep:
                            r = r + d
                        else:
                            q_buf[p, j] = q
                        r_buf[p, j] = r
                    if last_sweep:
                        if is_own:
                            x = x_buf[p, j] + d
                            if not last:
                                x_buf[p, j] = x
                            out_nat[section, p - OFF, pl.ds(j, SUB, stride=jn), :] = x
                    else:
                        d_buf[p, j] = d

            def update_own(p, carry):
                update(p, True)
                return carry

            own(update_own, 0)
            if not last:
                both_halos(width, lambda p: update(p, False))
        pltpu.make_async_copy(out_nat.at[section], out_hbm.at[0, section], out_sem.at[section]).start()

    for section in range(STEPS):
        pltpu.make_async_copy(out_nat.at[section], out_hbm.at[0, section], out_sem.at[section]).wait()
    k_halo[2]()
    f_halo[2]()

    @pl.when(tm < nt - 1)
    def _():
        corr.wait_send()


def solution(mesh):
    nt, ns = mesh.shape["tm"], mesh.shape["space"]

    def body(c_points, corrections, conductivity, forcing):
        depth, rows, lanes = conductivity.shape
        planes = depth + 2 * OFF
        jn = rows // SUB
        nat = pltpu.VMEM((depth, rows, lanes), jnp.float32)
        wide = pltpu.VMEM((planes, rows, lanes), jnp.float32)
        tiles = pltpu.VMEM((planes, jn, SUB, lanes), jnp.float32)
        dma = pltpu.SemaphoreType.DMA
        stages = STEPS * ITERS
        return pl.pallas_call(
            functools.partial(kernel, nt, ns, depth, rows),
            out_shape=jax.ShapeDtypeStruct((1, STEPS, depth, rows, lanes), jnp.float32),
            in_specs=[pl.BlockSpec(memory_space=pl.ANY)] * 4,
            out_specs=pl.BlockSpec(memory_space=pl.ANY),
            scratch_shapes=[
                nat, nat, wide, wide,
                pltpu.VMEM((STEPS, depth, rows, lanes), jnp.float32),
                tiles, tiles, tiles, tiles, tiles, tiles,
                tiles, tiles, tiles, tiles,
                pltpu.VMEM((stages, ns, SUB, lanes), jnp.float32),
                pltpu.VMEM((stages, SUB, lanes), jnp.float32),
                dma((3,)), dma((STEPS,)), dma, dma, dma((6,)), dma((6,)),
                dma((stages, ns)), dma((stages, ns)),
            ],
            compiler_params=pltpu.CompilerParams(
                collective_id=0, has_side_effects=True, vmem_limit_bytes=48 * 1024 * 1024),
        )(c_points, corrections, conductivity, forcing)

    in_specs = (
        P("tm", "space", None, None),
        P("tm", "space", None, None),
        P("space", None, None),
        P("space", None, None),
    )
    out_specs = P("tm", None, "space", None, None)
    return jax.shard_map(body, mesh=mesh, in_specs=in_specs, out_specs=out_specs, check_vma=False)
```

```python
import functools

import jax
import jax.numpy as jnp
from jax import lax
from jax.experimental import pallas as pl
from jax.experimental.pallas import tpu as pltpu
from jax.sharding import PartitionSpec as P

ITERS = 6
STEPS = 2
STEP_RATE = 4.0
SOURCE_WEIGHT = 0.25
HALO = ITERS * STEPS + 1
OFF = HALO + 1
SUB = 8


def kernel(nt, ns, depth, rows, c_hbm, corr_hbm, cond_hbm, f_hbm, out_hbm,
           c_nat, g_nat, k_nat, f_nat, out_nat, x_buf, r_buf, w_buf, p_buf, q_buf, d_buf, t_buf, o_buf,
           dg, cx, cy, cz, slots, totals,
           in_sem, out_sem, corr_send, corr_recv, halo_send, halo_recv, red_send, red_recv):
    tm = lax.axis_index("tm")
    me = lax.axis_index("space")
    jn = rows // SUB
    top = OFF + depth
    planes = top + OFF
    half = 0.5 * STEP_RATE

    loads = [
        pltpu.make_async_copy(cond_hbm, k_nat.at[pl.ds(OFF, depth)], in_sem.at[0]),
        pltpu.make_async_copy(c_hbm.at[0], c_nat, in_sem.at[1]),
        pltpu.make_async_copy(f_hbm, f_nat.at[pl.ds(OFF, depth)], in_sem.at[2]),
    ]
    for load in loads:
        load.start()

    barrier = pltpu.get_barrier_semaphore()
    for other in range(1, ns):
        pl.semaphore_signal(barrier, inc=1, device_id={"space": lax.rem(me + other, ns)})

    @pl.when(tm > 0)
    def _():
        pl.semaphore_signal(barrier, inc=1, device_id={"tm": tm - 1})

    pl.semaphore_wait(barrier, ns - 1 + jnp.where(tm < nt - 1, 1, 0))

    corr = pltpu.make_async_remote_copy(
        src_ref=corr_hbm.at[0], dst_ref=g_nat, send_sem=corr_send, recv_sem=corr_recv,
        device_id={"tm": jnp.minimum(tm + 1, nt - 1)})

    @pl.when(tm < nt - 1)
    def _():
        corr.start()

    def halo(src, src_off, dst, width, slot):
        up = pltpu.make_async_remote_copy(
            src_ref=src.at[pl.ds(src_off + depth - width, width)],
            dst_ref=dst.at[pl.ds(OFF - width, width)],
            send_sem=halo_send.at[2 * slot], recv_sem=halo_recv.at[2 * slot],
            device_id={"space": jnp.minimum(me + 1, ns - 1)})
        down = pltpu.make_async_remote_copy(
            src_ref=src.at[pl.ds(src_off, width)],
            dst_ref=dst.at[pl.ds(top, width)],
            send_sem=halo_send.at[2 * slot + 1], recv_sem=halo_recv.at[2 * slot + 1],
            device_id={"space": jnp.maximum(me - 1, 0)})

        def start():
            pl.when(me < ns - 1)(up.start)
            pl.when(me > 0)(down.start)

        def wait():
            pl.when(me > 0)(up.wait_recv)
            pl.when(me < ns - 1)(down.wait_recv)

        def wait_send():
            pl.when(me < ns - 1)(up.wait_send)
            pl.when(me > 0)(down.wait_send)

        return start, wait, wait_send

    k_halo = halo(cond_hbm, 0, k_nat, HALO, 0)
    f_halo = halo(f_hbm, 0, f_nat, HALO - 1, 1)
    x_halo = halo(x_buf, OFF, x_buf, HALO, 2)
    k_halo[0]()
    f_halo[0]()

    zero_plane = jnp.zeros((rows, 128), jnp.float32)
    zero_tiles = jnp.zeros((jn, SUB, 128), jnp.float32)

    def clear(lo, count):
        def one(i, carry):
            k_nat[lo + i] = zero_plane
            f_nat[lo + i] = zero_plane
            x_buf[lo + i] = zero_tiles
            return carry
        lax.fori_loop(0, count, one, 0)

    clear(0, 1)
    clear(planes - 1, 1)
    pl.when(me == 0)(lambda: clear(1, HALO))
    pl.when(me == ns - 1)(lambda: clear(top, HALO))

    for buf in (r_buf, w_buf):
        buf[0] = zero_tiles
        buf[1] = zero_tiles
        buf[planes - 2] = zero_tiles
        buf[planes - 1] = zero_tiles

    lane = lax.broadcasted_iota(jnp.int32, (SUB, 128), 1)
    sub = lax.broadcasted_iota(jnp.int32, (SUB, 128), 0)
    inner_lane = jnp.where(lane < 127, 1.0, 0.0)
    first_lane = jnp.where(lane > 0, 1.0, 0.0)
    inner_sub = jnp.where(sub < SUB - 1, 1.0, 0.0)
    first_sub = jnp.where(sub > 0, 1.0, 0.0)

    def nat(ref, p, j):
        return ref[p, pl.ds(j, SUB, stride=jn), :]

    def ahead(x):
        return pltpu.roll(x, 127, 1)

    def behind(x):
        return pltpu.roll(x, 1, 1)

    def sub_ahead(x):
        return pltpu.roll(x, SUB - 1, 0)

    def sub_behind(x):
        return pltpu.roll(x, 1, 0)

    loads[0].wait()
    k_halo[1]()

    def make_weights(i, carry):
        p = i + 1
        k = [nat(k_nat, p, j) for j in range(jn)]
        up = [nat(k_nat, p + 1, j) for j in range(jn)]
        dn = [nat(k_nat, p - 1, j) for j in range(jn)]
        z = me * depth + p - OFF
        face = jnp.where((z >= 0) & (z + 1 < ns * depth), -half, 0.0)
        for j in range(jn):
            right = ahead(k[j]) * inner_lane
            left = behind(k[j]) * first_lane
            yp = k[j + 1] if j + 1 < jn else sub_ahead(k[0]) * inner_sub
            ym = k[j - 1] if j > 0 else sub_behind(k[jn - 1]) * first_sub
            around = right + left + yp + ym + up[j] + dn[j]
            dg[p, j] = 1.0 + half * (6.0 * k[j] + around)
            cx[p, j] = -half * (k[j] + right) * inner_lane
            wy = -half * (k[j] + yp)
            cy[p, j] = wy if j + 1 < jn else wy * inner_sub
            cz[p, j] = face * (k[j] + up[j])
        return carry

    lax.fori_loop(0, planes - 2, make_weights, 0)

    def apply(ref, p):
        v = [ref[p, j] for j in range(jn)]
        c = [cx[p, j] for j in range(jn)]
        y = [cy[p, j] for j in range(jn)]
        rolled = [ahead(v[j]) for j in range(jn)]
        back = [behind(c[j] * v[j]) for j in range(jn)]
        out = []
        for j in range(jn):
            acc = dg[p, j] * v[j] + cz[p, j] * ref[p + 1, j] + cz[p - 1, j] * ref[p - 1, j]
            acc = acc + y[j] * (v[j + 1] if j + 1 < jn else sub_ahead(v[0]))
            acc = acc + (y[j - 1] * v[j - 1] if j > 0 else sub_behind(y[jn - 1] * v[jn - 1]))
            out.append(acc + (c[j] * rolled[j] + back[j]))
        return out, v

    def both_halos(width, fn):
        count = (width + 1) // 2

        def step(i, carry):
            for t in range(2):
                fn(OFF - 1 - (2 * i + t))
                fn(top + 2 * i + t)
            return carry
        if count:
            lax.fori_loop(0, count, step, 0)

    def own(fn, carry, chunk=4):
        def step(i, carry):
            for t in range(chunk):
                carry = fn(OFF + i * chunk + t, carry)
            return carry
        return lax.fori_loop(0, depth // chunk, step, carry)

    loads[1].wait()

    @pl.when(tm > 0)
    def _():
        corr.wait_recv()

        def add(p, carry):
            for j in range(jn):
                x_buf[p, j] = nat(c_nat, p - OFF, j) + nat(g_nat, p - OFF, j)
            return carry
        own(add, 0)

    @pl.when(tm == 0)
    def _():
        def add(p, carry):
            for j in range(jn):
                x_buf[p, j] = nat(c_nat, p - OFF, j)
            return carry
        own(add, 0)

    x_halo[0]()
    loads[2].wait()
    f_halo[1]()

    def first_residual(p):
        image, v = apply(x_buf, p)
        for j in range(jn):
            r_buf[p, j] = (v[j] + SOURCE_WEIGHT * nat(f_nat, p, j)) - image[j]

    def first_own(i, carry):
        for t in range(2):
            first_residual(OFF + 1 + 2 * i + t)
        return carry

    lax.fori_loop(0, (depth - 2) // 2, first_own, 0)
    x_halo[1]()
    x_halo[2]()
    first_residual(OFF)
    first_residual(top - 1)
    both_halos(HALO - 1, first_residual)

    def spread(row):
        return jnp.broadcast_to(row, (SUB, 128))

    def reduce(stage, parts):
        for i, part in enumerate(parts):
            slots[stage, me, i:i + 1] = jnp.sum(part, axis=0, keepdims=True)
        for i in range(len(parts), SUB):
            slots[stage, me, i:i + 1] = jnp.zeros((1, 128), jnp.float32)
        copies = []
        for other in range(1, ns):
            copies.append(pltpu.make_async_remote_copy(
                src_ref=slots.at[stage, me], dst_ref=slots.at[stage, me],
                send_sem=red_send.at[stage, other], recv_sem=red_recv.at[stage, other],
                device_id={"space": lax.rem(me + other, ns)}))
        for copy in copies:
            copy.start()
        for copy in copies:
            copy.wait()
        total = slots[stage, 0]
        for i in range(1, ns):
            total = total + slots[stage, i]
        totals[stage] = jnp.broadcast_to(jnp.sum(total, axis=1, keepdims=True), (SUB, 128))
        return [spread(totals[stage, i:i + 1]) for i in range(len(parts))]

    zero = jnp.zeros((SUB, 128), jnp.float32)
    for section in range(STEPS):
        for pair in range(ITERS // 2):
            n = section * (ITERS // 2) + pair
            width = HALO - 3 - 2 * n
            fresh = pair == 0

            def image_at(p):
                image, _ = apply(r_buf, p)
                for j in range(jn):
                    w_buf[p, j] = image[j]

            def image_own(p, carry):
                image_at(p)
                return carry

            own(image_own, 0)
            both_halos(width + 1, image_at)

            def twice_at(p):
                image, v = apply(w_buf, p)
                for j in range(jn):
                    t_buf[p, j] = image[j]
                return image, v

            def twice_own(p, sums):
                t, w = twice_at(p)
                sums = list(sums)
                for j in range(jn):
                    r = r_buf[p, j]
                    terms = [r * r, r * w[j], w[j] * w[j], w[j] * t[j]]
                    if not fresh:
                        q = q_buf[p, j]
                        z = (o_buf[p, j] - w[j]) * inverse
                        terms += [w[j] * q, q * q, t[j] * q, q * z]
                    sums = [total + term for total, term in zip(sums, terms)]
                return tuple(sums)

            sums = own(twice_own, (zero,) * (4 if fresh else 8))
            both_halos(width, twice_at)
            dots = reduce(n, sums)
            rr, rw, ww, wt = dots[:4]
            if fresh:
                beta = None
                alpha = rr / rw
                wq, qq, qz = ww, ww, wt
            else:
                wq_old, qq_old, tq_old, qz_old = dots[4:]
                beta = rr / norm_before
                alpha = rr / (rw - beta * rr * inverse)
                wq = ww + beta * wq_old
                qq = wq + beta * (wq_old + beta * qq_old)
                qz = wt + beta * (2.0 * tq_old + beta * qz_old)
            norm = alpha * alpha * qq - rr
            beta_next = norm / rr
            along = rw + alpha * (alpha * qz - 2.0 * wq)
            alpha_next = norm / (along - beta_next * norm / alpha)
            inverse_before = None if fresh else inverse
            inverse = 1.0 / alpha_next
            norm_before = norm
            last_pair = pair + 1 == ITERS // 2
            last = last_pair and section + 1 == STEPS

            def update(p, is_own):
                for j in range(jn):
                    r, w, t = r_buf[p, j], w_buf[p, j], t_buf[p, j]
                    if fresh:
                        pp, q, z = r, w, t
                    else:
                        pp = r + beta * p_buf[p, j]
                        q = w + beta * q_buf[p, j]
                        z = t + beta * ((o_buf[p, j] - w) * inverse_before)
                    r = r - alpha * q
                    p_next = r + beta_next * pp
                    d = alpha * pp + alpha_next * p_next
                    if not fresh:
                        d = d_buf[p, j] + d
                    if not last:
                        w = w - alpha * z
                        q = w + beta_next * q
                        r = r - alpha_next * q
                        r_buf[p, j] = r + d if last_pair else r
                    if not last_pair:
                        p_buf[p, j] = p_next
                        q_buf[p, j] = q
                        o_buf[p, j] = w
                        d_buf[p, j] = d
                    elif is_own:
                        x = x_buf[p, j] + d
                        if not last:
                            x_buf[p, j] = x
                        out_nat[section, p - OFF, pl.ds(j, SUB, stride=jn), :] = x

            def update_own(p, carry):
                update(p, True)
                return carry

            own(update_own, 0)
            if not last:
                both_halos(width, lambda p: update(p, False))
        pltpu.make_async_copy(out_nat.at[section], out_hbm.at[0, section], out_sem.at[section]).start()

    for section in range(STEPS):
        pltpu.make_async_copy(out_nat.at[section], out_hbm.at[0, section], out_sem.at[section]).wait()
    k_halo[2]()
    f_halo[2]()

    @pl.when(tm < nt - 1)
    def _():
        corr.wait_send()


def solution(mesh):
    nt, ns = mesh.shape["tm"], mesh.shape["space"]

    def body(c_points, corrections, conductivity, forcing):
        depth, rows, lanes = conductivity.shape
        planes = depth + 2 * OFF
        jn = rows // SUB
        nat = pltpu.VMEM((depth, rows, lanes), jnp.float32)
        wide = pltpu.VMEM((planes, rows, lanes), jnp.float32)
        tiles = pltpu.VMEM((planes, jn, SUB, lanes), jnp.float32)
        dma = pltpu.SemaphoreType.DMA
        stages = STEPS * (ITERS // 2)
        return pl.pallas_call(
            functools.partial(kernel, nt, ns, depth, rows),
            out_shape=jax.ShapeDtypeStruct((1, STEPS, depth, rows, lanes), jnp.float32),
            in_specs=[pl.BlockSpec(memory_space=pl.ANY)] * 4,
            out_specs=pl.BlockSpec(memory_space=pl.ANY),
            scratch_shapes=[
                nat, nat, wide, wide,
                pltpu.VMEM((STEPS, depth, rows, lanes), jnp.float32),
                tiles, tiles, tiles, tiles, tiles, tiles, tiles, tiles,
                tiles, tiles, tiles, tiles,
                pltpu.VMEM((stages, ns, SUB, lanes), jnp.float32),
                pltpu.VMEM((stages, SUB, lanes), jnp.float32),
                dma((3,)), dma((STEPS,)), dma, dma, dma((6,)), dma((6,)),
                dma((stages, ns)), dma((stages, ns)),
            ],
            compiler_params=pltpu.CompilerParams(
                collective_id=0, has_side_effects=True, vmem_limit_bytes=48 * 1024 * 1024),
        )(c_points, corrections, conductivity, forcing)

    in_specs = (
        P("tm", "space", None, None),
        P("tm", "space", None, None),
        P("space", None, None),
        P("space", None, None),
    )
    out_specs = P("tm", None, "space", None, None)
    return jax.shard_map(body, mesh=mesh, in_specs=in_specs, out_specs=out_specs, check_vma=False)
```
